32 devices in a mesh: groups: 2 (over y), adapter: 4 (over x, core), tensor: 4 (over z).
Axes of the slice: x: 2, y: 2, z: 4, core: 2. Of those that a mesh axis runs over, the one named last changes fastest.
Arguments:
- tokens: bfloat16 [2048, 8192], P(('groups', 'adapter'), 'tensor'), parts along dimension 0, may hold values from -6 to 6
- query_weight: bfloat16 [8192, 8192], P('tensor', 'adapter'), may hold values from -0.0625 to 0.0625
- adapter_down_weight: bfloat16 [128, 16, 8192], P('adapter', None, 'tensor'), may hold values from -0.0625 to 0.0625
- adapter_up_weight: bfloat16 [128, 16, 8192], P('adapter'), may hold values from -1.5 to 1.5
- block_adapter_ids: int32 [16], P('groups'), parts along dimension 0, may hold values from 0 to 127, as said below
- block_live_count: int32 [16], P('groups'), parts along dimension 0, may hold values from 1 to 128
- adapter_slot_index: int32 [256], P('groups'), parts along dimension 0, may hold values from 0 to 127, as said below
Outputs:
- query: bfloat16 [2048, 8192], P(('groups', 'tensor'), 'adapter'), parts along dimension 0
The draws below stay inside these ranges and needn't reach their ends.
There are 2 independent parts, one for each index of `groups`. The reference program is written for one: setup_inputs(seed, part) draws one part's arguments, and reference() takes and returns one part's arrays. A program takes and returns all parts, laid end to end along the dimension named above; an argument that names none is the same for every part. Nothing has to cross between parts.
Inputs may be any that keep to these rules, and one draw needn't show every extreme that they name: Counting blocks by the owner range adapter_slot_index[block_adapter_ids[k]] // 32, no owner has more than 4 blocks, and one owner has exactly 4 in every draw. `adapter_slot_index`: A permutation: each slot holds exactly one adapter.
All inputs are finite; a program needn't handle non-finite values.
Results may differ from the reference program's by a relative error of at most 0.014.
Values may be sent and summed in bfloat16 or wider, within the bound.
A program may use at most 128 MiB of HBM per device.

```python
import jax
import jax.numpy as jnp

MODEL_WIDTH = 8192
QUERY_OUTPUTS = 8192
ADAPTER_RANK = 16
ADP_DEV = 32
BLOCK = 128
ADAPTER_COUNT = 128
FEAT = 2048
CAP = 4
BLOCKS = 8
TOKENS = 1024


def plan_draw(key):
    owner_count = ADAPTER_COUNT // ADP_DEV
    slot_table = jax.random.permutation(jax.random.fold_in(key, 101), jnp.arange(ADAPTER_COUNT, dtype=jnp.int32)).astype(jnp.int32)
    holder = jnp.argsort(slot_table, stable=True).astype(jnp.int32)
    hottest = jax.random.randint(jax.random.fold_in(key, 102), (), 0, owner_count, dtype=jnp.int32)
    seat_owner = jnp.arange((owner_count - 1) * CAP, dtype=jnp.int32) // CAP
    seat_owner = seat_owner + (seat_owner >= hottest).astype(jnp.int32)
    seat_owner = jax.random.permutation(jax.random.fold_in(key, 103), seat_owner)[:BLOCKS - CAP]
    owner_list = jnp.concatenate([jnp.full((CAP,), hottest, jnp.int32), seat_owner.astype(jnp.int32)])
    owner_list = jax.random.permutation(jax.random.fold_in(key, 104), owner_list)
    local_slot = jax.random.randint(jax.random.fold_in(key, 105), (BLOCKS,), 0, ADP_DEV, dtype=jnp.int32)
    adapters = holder[owner_list * ADP_DEV + local_slot]
    return (slot_table, adapters.astype(jnp.int32))


def draw_block_adapter_ids(key, part):
    return plan_draw(key)[1]


def draw_adapter_slot_index(key, part):
    return plan_draw(key)[0]


def touch_ends(drawn, stream_key, low, top_value):
    longest = drawn.shape.index(max(drawn.shape))
    spots = []
    for shift in (0, 1):
        where = [jax.random.randint(jax.random.fold_in(stream_key, axis), (), 0, length) for axis, length in enumerate(drawn.shape)]
        where[longest] = (where[longest] + shift) % drawn.shape[longest]
        spots.append(tuple(where))
    return drawn.at[spots[0]].set(low).at[spots[1]].set(top_value)


def levels(own_key, dims, cuts, low, largest):
    def one(position, blocks):
        draws = jax.random.uniform(jax.random.fold_in(jax.random.fold_in(own_key, 6), position), (blocks,), jnp.float32, low / len(cuts), largest / len(cuts))
        return jnp.repeat(jnp.exp(draws), dims[position] // blocks).reshape((-1,) + (1,) * (len(dims) - position - 1))

    factor_of = one(*cuts[0])
    for cut in cuts[1:]:
        factor_of = factor_of * one(*cut)
    return factor_of


def normal_values(rng, extent, spread, reach, pieces=(), held_as=jnp.bfloat16):
    array = spread * jax.random.normal(rng, extent, jnp.float32)
    if pieces:
        array = array * levels(rng, extent, pieces, -0.22, 0.18)
    return jnp.clip(array, -reach, reach).astype(held_as)


def setup_inputs(seed: int = 0, part: int = 0) -> dict:
    key_list = jax.random.split(jax.random.key(seed), 8)
    own_keys = jax.random.split(jax.random.fold_in(key_list[7], part), 8)
    tokens = normal_values(own_keys[0], (TOKENS, MODEL_WIDTH), 1.0, 6.0, ((0, 4), (1, 4)))
    query_weight = normal_values(key_list[1], (MODEL_WIDTH, QUERY_OUTPUTS), MODEL_WIDTH ** -0.5, 0.0625, ((0, 4), (1, 4)))
    adapter_down_weight = normal_values(key_list[2], (ADAPTER_COUNT, ADAPTER_RANK, MODEL_WIDTH), MODEL_WIDTH ** -0.5, 0.0625, ((0, 4), (2, 4)))
    adapter_up_weight = normal_values(key_list[3], (ADAPTER_COUNT, ADAPTER_RANK, QUERY_OUTPUTS), ADAPTER_RANK ** -0.5, 1.5, ((0, 4),))
    block_adapter_ids = draw_block_adapter_ids(jax.random.fold_in(jax.random.fold_in(key_list[7], part), 71), part)
    block_live_count = touch_ends(jax.random.randint(own_keys[5], (BLOCKS,), 1, BLOCK + 1), jax.random.fold_in(own_keys[5], 1), 1, BLOCK).astype(jnp.int32)
    adapter_slot_index = draw_adapter_slot_index(jax.random.fold_in(jax.random.fold_in(key_list[7], part), 71), part)
    return dict(tokens=tokens, query_weight=query_weight, adapter_down_weight=adapter_down_weight, adapter_up_weight=adapter_up_weight, block_adapter_ids=block_adapter_ids, block_live_count=block_live_count, adapter_slot_index=adapter_slot_index)


def reference(tokens, query_weight, adapter_down_weight, adapter_up_weight, block_adapter_ids, block_live_count, adapter_slot_index):
    block_slot_index = adapter_slot_index[block_adapter_ids].astype(jnp.int32)
    down_weight_blocks = adapter_down_weight[block_slot_index].astype(jnp.float32)
    up_weight_blocks = adapter_up_weight[block_slot_index].astype(jnp.float32)
    positions = jnp.arange(BLOCK, dtype=jnp.int32)
    live_mask = (positions[None, :] < block_live_count[:, None]).astype(jnp.float32)
    token_blocks = tokens.reshape(BLOCKS, BLOCK, MODEL_WIDTH).astype(jnp.float32)
    total = jnp.zeros((TOKENS, QUERY_OUTPUTS), jnp.float32)
    for slice_index in range(MODEL_WIDTH // FEAT):
        low_edge = slice_index * FEAT
        high_edge = low_edge + FEAT
        shrunk = jnp.einsum("ksd,krd->ksr", token_blocks[:, :, low_edge:high_edge], down_weight_blocks[:, :, low_edge:high_edge])
        shrunk = (shrunk * live_mask[:, :, None]).astype(jnp.bfloat16)
        adapter_part = jnp.einsum("ksr,krf->ksf", shrunk.astype(jnp.float32), up_weight_blocks).reshape(TOKENS, QUERY_OUTPUTS)
        base_part = jnp.dot(tokens[:, low_edge:high_edge], query_weight[low_edge:high_edge, :], preferred_element_type=jnp.float32)
        partial_value = (base_part + 2.0 * adapter_part).astype(jnp.bfloat16)
        total = total + partial_value.astype(jnp.float32)
    return total.astype(jnp.bfloat16)
```

```python
import functools

import jax
import jax.numpy as jnp
from jax import lax
from jax.experimental import pallas as pl
from jax.experimental.pallas import tpu as pltpu
from jax.sharding import PartitionSpec as P

BLOCK = 128
SCALE = 2.0
MESH = pl.DeviceIdType.MESH


def kernel(
    A, T,
    ids, live, slots, tok_hbm, w_hbm, dn_hbm, up_hbm, out_ref,
    tok, w, dn, up, buf_r, buf_l, acc, dn_send, dn_recv, up_send, up_recv, s_send, s_recv,
    ld_sem, w_sem, tok_ss, tok_rs, dn_ss, dn_rs, up_ss, up_rs, s_ss, s_rs,
    r_ss, r_rs, l_ss, l_rs,
):
    a = lax.axis_index("adapter")
    t = lax.axis_index("tensor")
    chips = A // 2
    x, core = a // 2, a % 2
    partner = 2 * x + 1 - core
    rows_a = tok_hbm.shape[0]
    rows = rows_a * A
    rows_d = rows // T
    per_dev = dn_hbm.shape[0]
    np_, _, cp = buf_r.shape[1:]
    cols = np_ * cp
    nb_a = rows_a // BLOCK
    nb_t = rows_d // BLOCK

    def local(src, dst, i):
        return pltpu.make_async_copy(src, dst, ld_sem.at[i])

    my_rows = tok.at[pl.ds(pl.multiple_of(a * rows_a, rows_a), rows_a)]
    tok_load = local(tok_hbm, my_rows, 0)
    dn_load = local(dn_hbm, dn, 1)
    up_load = local(up_hbm, up, 2)
    tok_load.start()
    dn_load.start()

    def w_load(p):
        c = pl.ds(pl.multiple_of(p * cp, cp), cp)
        return pltpu.make_async_copy(w_hbm.at[:, c], w.at[p], w_sem.at[p])

    for p in range(np_):
        w_load(p).start()
    up_load.start()

    barrier = pltpu.get_barrier_semaphore()
    for i in range(1, A * T):
        q = (a * T + t + i) % (A * T)
        pl.semaphore_signal(
            barrier, inc=1, device_id={"adapter": q // T, "tensor": q % T}, device_id_type=MESH
        )
    pl.semaphore_wait(barrier, A * T - 1)

    def tok_copy(owner, to, ssem):
        r = tok.at[pl.ds(pl.multiple_of(owner * rows_a, rows_a), rows_a)]
        return pltpu.make_async_remote_copy(
            r, r, tok_ss.at[ssem], tok_rs.at[owner],
            device_id={"adapter": to}, device_id_type=MESH,
        )

    tok_load.wait()
    sends = [tok_copy(a, partner, 0)]
    for i in range(1, chips):
        sends.append(tok_copy(a, 2 * ((x + i) % chips) + core, i))
    for c in sends:
        c.start()

    def slot_of(k):
        return slots[ids[k]]

    dn_load.wait()
    for i in range(A):
        for b in range(nb_a):
            dn_send[i, b] = dn[lax.rem(slot_of(i * nb_a + b), per_dev)]
    dn_recv[a] = dn_send[a]

    def dn_copy(i):
        to = (a + i) % A
        return pltpu.make_async_remote_copy(
            dn_send.at[to], dn_recv.at[a], dn_ss.at[i], dn_rs.at[i],
            device_id={"adapter": to}, device_id_type=MESH,
        )

    for i in range(1, A):
        dn_copy(i).start()

    local_chunks = (2 * rows_a) // rows_d
    aligned = (2 * rows_a) % rows_d == 0 and local_chunks >= 2
    high = jnp.maximum((2 * (x + 1) * rows_a - 1) // rows_d, 1)
    low = jnp.minimum((2 * x * rows_a) // rows_d, T - 2)

    def order_r(j):
        v = T - j
        v = jnp.where(v <= high, v - 1, v)
        return jnp.where(j == 0, high, v)

    def order_l(j):
        v = j - 1
        v = jnp.where(v >= low, v + 1, v)
        return jnp.where(j == 0, low, v)

    pos_r = jnp.where(t == high, 0, jnp.where(t > high, T - t, T - 1 - t))
    pos_l = jnp.where(t == low, 0, jnp.where(t < low, t + 1, t))

    def base(d, p):
        return jnp.dot(
            tok[pl.ds(pl.multiple_of(d * rows_d, rows_d), rows_d), :], w[p],
            preferred_element_type=jnp.float32,
        )

    def flow(buf, ss, rs, to, j, p):
        return pltpu.make_async_remote_copy(
            buf.at[j, p], buf.at[j, p], ss.at[j, p], rs.at[j, p],
            device_id={"tensor": to}, device_id_type=MESH,
        )

    right, left = (t + 1) % T, (t + T - 1) % T

    def step(buf, ss, rs, to, d, j, p, fresh):
        @pl.when(fresh)
        def _():
            buf[j, p] = base(d, p).astype(buf.dtype)

        @pl.when(jnp.logical_not(fresh))
        def _():
            mine = base(d, p)
            flow(buf, ss, rs, to, j, p).wait_recv()
            buf[j, p] = (mine + buf[j, p].astype(jnp.float32)).astype(buf.dtype)

        flow(buf, ss, rs, to, j, p).start()

    def wait_tokens(first):
        for i in range(1, chips):
            o = 2 * ((x + i) % chips) + core
            tok_copy(o, partner, 0).wait_recv()
            tok_copy(o, partner, chips + i - 1).start()
        for i in range(1, chips):
            o = 2 * ((x + i) % chips) + 1 - core
            tok_copy(o, partner, 0).wait_recv()

    def up_copy(i):
        to = (a + i) % A
        return pltpu.make_async_remote_copy(
            up_send.at[to], up_recv.at[a], up_ss.at[i], up_rs.at[i],
            device_id={"adapter": to}, device_id_type=MESH,
        )

    def s_dest(b):
        k = a * nb_a + b
        return k // nb_t, k % nb_t

    def s_copy(i, b):
        d, kk = s_dest(b)
        return pltpu.make_async_remote_copy(
            s_send.at[b], s_recv.at[t, kk], s_ss.at[i, b], s_rs.at[t, kk],
            device_id={"adapter": (a + i) % A, "tensor": d}, device_id_type=MESH,
        )

    def send_adapters():
        up_load.wait()
        for b in range(nb_t):
            sl = lax.rem(slot_of(t * nb_t + b), per_dev)
            for i in range(A):
                up_send[i, b] = up[sl, :, i * cols:(i + 1) * cols]
        up_recv[a] = up_send[a]
        for i in range(1, A):
            up_copy(i).start()
        for i in range(1, A):
            dn_copy(i).wait_recv()
        for b in range(nb_a):
            k = a * nb_a + b
            mine = dn_recv[lax.div(slot_of(k), per_dev), b]
            rows_b = tok[pl.ds(pl.multiple_of(k * BLOCK, BLOCK), BLOCK), :]
            s = lax.dot_general(
                mine, rows_b, (((1,), (1,)), ((), ())), preferred_element_type=jnp.float32
            )
            keep = lax.broadcasted_iota(jnp.int32, s.shape, 1) < live[k]
            s_send[b] = jnp.where(keep, s, 0.0).astype(s_send.dtype)
            d, kk = s_dest(b)
            for i in range(A):
                if i:
                    s_copy(i, b).start()
                else:
                    @pl.when(d == t)
                    def _():
                        s_recv[t, kk] = s_send[b]

                    @pl.when(d != t)
                    def _():
                        s_copy(0, b).start()

    def wait_adapters():
        for i in range(1, A):
            up_copy(i).wait_recv()
        for b in range(nb_t):
            owner = (t * nb_t + b) // nb_a
            for tt in range(T):
                c = pltpu.make_async_remote_copy(
                    s_send.at[0], s_recv.at[tt, b], s_ss.at[0, 0], s_rs.at[tt, b],
                    device_id={"adapter": partner}, device_id_type=MESH,
                )

                @pl.when(jnp.logical_or(owner != a, t != tt))
                def _():
                    c.wait_recv()

    def add_adapters(p):
        for b in range(nb_t):
            own = lax.div(slot_of(t * nb_t + b), per_dev)
            u = up_recv[own, b, :, pl.ds(pl.multiple_of(p * cp, cp), cp)]
            lhs = s_recv[:, b].reshape(T * s_recv.shape[2], BLOCK)
            r = slice(b * BLOCK, (b + 1) * BLOCK)
            acc[p, r] = acc[p, r] + SCALE * lax.dot_general(
                lhs, jnp.concatenate([u] * T, axis=0), (((0,), (0,)), ((), ())),
                preferred_element_type=jnp.float32,
            )

    if not aligned:
        tok_copy(partner, partner, 0).wait_recv()
        wait_tokens(True)

    for j in range(T - 1):
        if j == 0 and aligned:
            tok_copy(partner, partner, 0).wait_recv()
        if j == min(1, T - 2):
            if aligned:
                wait_tokens(True)
            send_adapters()
        if j == T - 2:
            wait_adapters()
        d_r, d_l = order_r(j), order_l(j)

        def body(p, _):
            if j == 0:
                w_load(p).wait()

            @pl.when(d_r > t)
            def _():
                step(buf_r, r_ss, r_rs, right, d_r, j, p, t == 0)

            @pl.when(d_l < t)
            def _():
                step(buf_l, l_ss, l_rs, left, d_l, j, p, t == T - 1)

            if j == min(1, T - 2):
                acc[p] = base(t, p)
            if j == T - 2:
                add_adapters(p)
            return 0

        lax.fori_loop(0, np_, body, 0)

    def last(p, _):
        @pl.when(t > 0)
        def _():
            flow(buf_r, r_ss, r_rs, right, pos_r, p).wait_recv()
            acc[p] = acc[p] + buf_r[pos_r, p].astype(jnp.float32)

        @pl.when(t < T - 1)
        def _():
            flow(buf_l, l_ss, l_rs, left, pos_l, p).wait_recv()
            acc[p] = acc[p] + buf_l[pos_l, p].astype(jnp.float32)

        out_ref[:, pl.ds(pl.multiple_of(p * cp, cp), cp)] = acc[p].astype(out_ref.dtype)
        return 0

    lax.fori_loop(0, np_, last, 0)

    for c in sends:
        c.wait_send()
    for i in range(1, chips):
        tok_copy(a, partner, chips + i - 1).wait_send()
    for i in range(1, A):
        dn_copy(i).wait_send()
        up_copy(i).wait_send()
    for b in range(nb_a):
        d, _ = s_dest(b)
        for i in range(1, A):
            s_copy(i, b).wait_send()

        @pl.when(d != t)
        def _():
            s_copy(0, b).wait_send()
    for j in range(T - 1):
        d_r, d_l = order_r(j), order_l(j)

        def drain(p, _):
            @pl.when(d_r > t)
            def _():
                flow(buf_r, r_ss, r_rs, right, j, p).wait_send()

            @pl.when(d_l < t)
            def _():
                flow(buf_l, l_ss, l_rs, left, j, p).wait_send()
            return 0

        lax.fori_loop(0, np_, drain, 0)


def on_device(tokens, query_weight, down, up, ids, live, slots):
    A, T = lax.axis_size("adapter"), lax.axis_size("tensor")
    rows_a, feat = tokens.shape
    cols = query_weight.shape[1]
    rank = down.shape[1]
    rows_d = rows_a * A // T
    cp = min(256, cols)
    np_ = cols // cp
    nb_a, nb_t = rows_a // BLOCK, rows_d // BLOCK
    chips = A // 2
    bf, f32 = jnp.bfloat16, jnp.float32
    dma = pltpu.SemaphoreType.DMA
    smem = pl.BlockSpec(memory_space=pltpu.SMEM)
    hbm = pl.BlockSpec(memory_space=pl.ANY)
    return pl.pallas_call(
        functools.partial(kernel, A, T),
        out_shape=jax.ShapeDtypeStruct((rows_d, cols), bf),
        in_specs=[smem, smem, smem, hbm, hbm, hbm, hbm],
        out_specs=pl.BlockSpec(memory_space=pltpu.VMEM),
        scratch_shapes=[
            pltpu.VMEM((rows_a * A, feat), bf),
            pltpu.VMEM((np_, feat, cp), bf),
            pltpu.VMEM(down.shape, bf),
            pltpu.VMEM(up.shape, bf),
            pltpu.VMEM((T - 1, np_, rows_d, cp), bf),
            pltpu.VMEM((T - 1, np_, rows_d, cp), bf),
            pltpu.VMEM((np_, rows_d, cp), f32),
            pltpu.VMEM((A, nb_a, rank, feat), bf),
            pltpu.VMEM((A, nb_a, rank, feat), bf),
            pltpu.VMEM((A, nb_t, rank, cols), bf),
            pltpu.VMEM((A, nb_t, rank, cols), bf),
            pltpu.VMEM((nb_a, rank, BLOCK), bf),
            pltpu.VMEM((T, nb_t, rank, BLOCK), bf),
            dma((3,)), dma((np_,)),
            dma((2 * chips,)), dma((A,)),
            dma((A,)), dma((A,)), dma((A,)), dma((A,)),
            dma((A, nb_a)), dma((T, nb_t)),
            dma((T - 1, np_)), dma((T - 1, np_)), dma((T - 1, np_)), dma((T - 1, np_)),
        ],
        compiler_params=pltpu.CompilerParams(
            collective_id=0, has_side_effects=True, vmem_limit_bytes=60 * 1024 * 1024
        ),
    )(ids, live, slots, tokens, query_weight, down, up)


def solution(mesh):
    placed = (
        P(("groups", "adapter"), "tensor"),
        P("tensor", "adapter"),
        P("adapter", None, "tensor"),
        P("adapter", None, None),
        P("groups"),
        P("groups"),
        P("groups"),
    )
    return jax.shard_map(
        on_device,
        mesh=mesh,
        in_specs=placed,
        out_specs=P(("groups", "tensor"), "adapter"),
        check_vma=False,
    )
```

```python
import functools

import jax
import jax.numpy as jnp
from jax import lax
from jax.experimental import pallas as pl
from jax.experimental.pallas import tpu as pltpu
from jax.sharding import PartitionSpec as P

BLOCK = 128
SCALE = 2.0
MESH = pl.DeviceIdType.MESH


def kernel(
    A, T,
    ids, live, slots, tok_hbm, w_hbm, dn_hbm, up_hbm, out_ref,
    tok, w, dn, up, buf_r, buf_l, acc, dn_send, dn_recv, up_send, up_recv, s_send, s_recv,
    ld_sem, w_sem, tok_ss, tok_rs, dn_ss, dn_rs, up_ss, up_rs, s_ss, s_rs,
    r_ss, r_rs, l_ss, l_rs,
):
    a = lax.axis_index("adapter")
    t = lax.axis_index("tensor")
    chips = A // 2
    x, core = a // 2, a % 2
    partner = 2 * x + 1 - core
    rows_a = tok_hbm.shape[0]
    rows = rows_a * A
    rows_d = rows // T
    per_dev = dn_hbm.shape[0]
    np_, _, cp = buf_r.shape[1:]
    cols = np_ * cp
    nb_a = rows_a // BLOCK
    nb_t = rows_d // BLOCK

    def local(src, dst, i):
        return pltpu.make_async_copy(src, dst, ld_sem.at[i])

    my_rows = tok.at[pl.ds(pl.multiple_of(a * rows_a, rows_a), rows_a)]
    tok_load = local(tok_hbm, my_rows, 0)
    dn_load = local(dn_hbm, dn, 1)
    up_load = local(up_hbm, up, 2)
    tok_load.start()
    dn_load.start()

    def w_load(p):
        c = pl.ds(pl.multiple_of(p * cp, cp), cp)
        return pltpu.make_async_copy(w_hbm.at[:, c], w.at[p], w_sem.at[p])

    for p in range(np_):
        w_load(p).start()
    up_load.start()

    barrier = pltpu.get_barrier_semaphore()
    for i in range(1, A * T):
        q = (a * T + t + i) % (A * T)
        pl.semaphore_signal(
            barrier, inc=1, device_id={"adapter": q // T, "tensor": q % T}, device_id_type=MESH
        )
    pl.semaphore_wait(barrier, A * T - 1)

    def tok_copy(owner, to, ssem):
        r = tok.at[pl.ds(pl.multiple_of(owner * rows_a, rows_a), rows_a)]
        return pltpu.make_async_remote_copy(
            r, r, tok_ss.at[ssem], tok_rs.at[owner],
            device_id={"adapter": to}, device_id_type=MESH,
        )

    tok_load.wait()
    sends = [tok_copy(a, partner, 0)]
    for i in range(1, chips):
        sends.append(tok_copy(a, 2 * ((x + i) % chips) + core, i))
    for c in sends:
        c.start()

    def slot_of(k):
        return slots[ids[k]]

    dn_load.wait()
    for i in range(A):
        for b in range(nb_a):
            dn_send[i, b] = dn[lax.rem(slot_of(i * nb_a + b), per_dev)]
    dn_recv[a] = dn_send[a]

    def dn_copy(i):
        to = (a + i) % A
        return pltpu.make_async_remote_copy(
            dn_send.at[to], dn_recv.at[a], dn_ss.at[i], dn_rs.at[i],
            device_id={"adapter": to}, device_id_type=MESH,
        )

    local_chunks = (2 * rows_a) // rows_d
    aligned = (2 * rows_a) % rows_d == 0 and local_chunks >= 2
    high = jnp.maximum((2 * (x + 1) * rows_a - 1) // rows_d, 1)
    low = jnp.minimum((2 * x * rows_a) // rows_d, T - 2)

    def order_r(j):
        v = T - j
        v = jnp.where(v <= high, v - 1, v)
        return jnp.where(j == 0, high, v)

    def order_l(j):
        v = j - 1
        v = jnp.where(v >= low, v + 1, v)
        return jnp.where(j == 0, low, v)

    pos_r = jnp.where(t == high, 0, jnp.where(t > high, T - t, T - 1 - t))
    pos_l = jnp.where(t == low, 0, jnp.where(t < low, t + 1, t))

    def base(d, p):
        return jnp.dot(
            tok[pl.ds(pl.multiple_of(d * rows_d, rows_d), rows_d), :], w[p],
            preferred_element_type=jnp.float32,
        )

    def flow(buf, ss, rs, to, j, p):
        return pltpu.make_async_remote_copy(
            buf.at[j, p], buf.at[j, p], ss.at[j, p], rs.at[j, p],
            device_id={"tensor": to}, device_id_type=MESH,
        )

    right, left = (t + 1) % T, (t + T - 1) % T

    def step(buf, ss, rs, to, d, j, p, fresh):
        @pl.when(fresh)
        def _():
            buf[j, p] = base(d, p).astype(buf.dtype)

        @pl.when(jnp.logical_not(fresh))
        def _():
            mine = base(d, p)
            flow(buf, ss, rs, to, j, p).wait_recv()
            buf[j, p] = (mine + buf[j, p].astype(jnp.float32)).astype(buf.dtype)

        flow(buf, ss, rs, to, j, p).start()

    def wait_tokens(first):
        for i in range(1, chips):
            o = 2 * ((x + i) % chips) + core
            tok_copy(o, partner, 0).wait_recv()
            tok_copy(o, partner, chips + i - 1).start()
        for i in range(1, chips):
            o = 2 * ((x + i) % chips) + 1 - core
            tok_copy(o, partner, 0).wait_recv()

    def up_copy(i):
        to = (a + i) % A
        return pltpu.make_async_remote_copy(
            up_send.at[to], up_recv.at[a], up_ss.at[i], up_rs.at[i],
            device_id={"adapter": to}, device_id_type=MESH,
        )

    def s_dest(b):
        k = a * nb_a + b
        return k // nb_t, k % nb_t

    def s_copy(i, b):
        d, kk = s_dest(b)
        return pltpu.make_async_remote_copy(
            s_send.at[b], s_recv.at[t, kk], s_ss.at[i, b], s_rs.at[t, kk],
            device_id={"adapter": (a + i) % A, "tensor": d}, device_id_type=MESH,
        )

    def send_adapters():
        up_load.wait()
        for b in range(nb_t):
            sl = lax.rem(slot_of(t * nb_t + b), per_dev)
            for i in range(A):
                up_send[i, b] = up[sl, :, i * cols:(i + 1) * cols]
        up_recv[a] = up_send[a]
        for i in range(1, A):
            up_copy(i).start()

    def send_shrunk():
        for i in range(1, A):
            dn_copy(i).wait_recv()
        for b in range(nb_a):
            k = a * nb_a + b
            mine = dn_recv[lax.div(slot_of(k), per_dev), b]
            rows_b = tok[pl.ds(pl.multiple_of(k * BLOCK, BLOCK), BLOCK), :]
            s = lax.dot_general(
                mine, rows_b, (((1,), (1,)), ((), ())), preferred_element_type=jnp.float32
            )
            keep = lax.broadcasted_iota(jnp.int32, s.shape, 1) < live[k]
            s_send[b] = jnp.where(keep, s, 0.0).astype(s_send.dtype)
            d, kk = s_dest(b)
            for i in range(A):
                if i:
                    s_copy(i, b).start()
                else:
                    @pl.when(d == t)
                    def _():
                        s_recv[t, kk] = s_send[b]

                    @pl.when(d != t)
                    def _():
                        s_copy(0, b).start()

    def wait_adapters():
        for i in range(1, A):
            up_copy(i).wait_recv()
        for b in range(nb_t):
            owner = (t * nb_t + b) // nb_a
            for tt in range(T):
                c = pltpu.make_async_remote_copy(
                    s_send.at[0], s_recv.at[tt, b], s_ss.at[0, 0], s_rs.at[tt, b],
                    device_id={"adapter": partner}, device_id_type=MESH,
                )

                @pl.when(jnp.logical_or(owner != a, t != tt))
                def _():
                    c.wait_recv()

    def add_adapters(p):
        for b in range(nb_t):
            own = lax.div(slot_of(t * nb_t + b), per_dev)
            u = up_recv[own, b, :, pl.ds(pl.multiple_of(p * cp, cp), cp)]
            lhs = s_recv[:, b].reshape(T * s_recv.shape[2], BLOCK)
            r = slice(b * BLOCK, (b + 1) * BLOCK)
            acc[p, r] = acc[p, r] + SCALE * lax.dot_general(
                lhs, jnp.concatenate([u] * T, axis=0), (((0,), (0,)), ((), ())),
                preferred_element_type=jnp.float32,
            )

    if not aligned:
        tok_copy(partner, partner, 0).wait_recv()
        wait_tokens(True)

    for j in range(T - 1):
        if j == 0 and aligned:
            tok_copy(partner, partner, 0).wait_recv()
        if j == min(1, T - 2):
            if aligned:
                wait_tokens(True)
            for i in range(1, A):
                dn_copy(i).start()
            send_adapters()
        if j == T - 2:
            send_shrunk()
        d_r, d_l = order_r(j), order_l(j)

        def body(p, _):
            if j == 0:
                w_load(p).wait()

            @pl.when(d_r > t)
            def _():
                step(buf_r, r_ss, r_rs, right, d_r, j, p, t == 0)

            @pl.when(d_l < t)
            def _():
                step(buf_l, l_ss, l_rs, left, d_l, j, p, t == T - 1)

            if j == min(1, T - 2):
                acc[p] = base(t, p)
            return 0

        lax.fori_loop(0, np_, body, 0)

    wait_adapters()

    def last(p, _):
        add_adapters(p)

        @pl.when(t > 0)
        def _():
            flow(buf_r, r_ss, r_rs, right, pos_r, p).wait_recv()
            acc[p] = acc[p] + buf_r[pos_r, p].astype(jnp.float32)

        @pl.when(t < T - 1)
        def _():
            flow(buf_l, l_ss, l_rs, left, pos_l, p).wait_recv()
            acc[p] = acc[p] + buf_l[pos_l, p].astype(jnp.float32)

        out_ref[:, pl.ds(pl.multiple_of(p * cp, cp), cp)] = acc[p].astype(out_ref.dtype)
        return 0

    lax.fori_loop(0, np_, last, 0)

    for c in sends:
        c.wait_send()
    for i in range(1, chips):
        tok_copy(a, partner, chips + i - 1).wait_send()
    for i in range(1, A):
        dn_copy(i).wait_send()
        up_copy(i).wait_send()
    for b in range(nb_a):
        d, _ = s_dest(b)
        for i in range(1, A):
            s_copy(i, b).wait_send()

        @pl.when(d != t)
        def _():
            s_copy(0, b).wait_send()
    for j in range(T - 1):
        d_r, d_l = order_r(j), order_l(j)

        def drain(p, _):
            @pl.when(d_r > t)
            def _():
                flow(buf_r, r_ss, r_rs, right, j, p).wait_send()

            @pl.when(d_l < t)
            def _():
                flow(buf_l, l_ss, l_rs, left, j, p).wait_send()
            return 0

        lax.fori_loop(0, np_, drain, 0)


def on_device(tokens, query_weight, down, up, ids, live, slots):
    A, T = lax.axis_size("adapter"), lax.axis_size("tensor")
    rows_a, feat = tokens.shape
    cols = query_weight.shape[1]
    rank = down.shape[1]
    rows_d = rows_a * A // T
    cp = min(256, cols)
    np_ = cols // cp
    nb_a, nb_t = rows_a // BLOCK, rows_d // BLOCK
    chips = A // 2
    bf, f32 = jnp.bfloat16, jnp.float32
    dma = pltpu.SemaphoreType.DMA
    smem = pl.BlockSpec(memory_space=pltpu.SMEM)
    hbm = pl.BlockSpec(memory_space=pl.ANY)
    return pl.pallas_call(
        functools.partial(kernel, A, T),
        out_shape=jax.ShapeDtypeStruct((rows_d, cols), bf),
        in_specs=[smem, smem, smem, hbm, hbm, hbm, hbm],
        out_specs=pl.BlockSpec(memory_space=pltpu.VMEM),
        scratch_shapes=[
            pltpu.VMEM((rows_a * A, feat), bf),
            pltpu.VMEM((np_, feat, cp), bf),
            pltpu.VMEM(down.shape, bf),
            pltpu.VMEM(up.shape, bf),
            pltpu.VMEM((T - 1, np_, rows_d, cp), bf),
            pltpu.VMEM((T - 1, np_, rows_d, cp), bf),
            pltpu.VMEM((np_, rows_d, cp), f32),
            pltpu.VMEM((A, nb_a, rank, feat), bf),
            pltpu.VMEM((A, nb_a, rank, feat), bf),
            pltpu.VMEM((A, nb_t, rank, cols), bf),
            pltpu.VMEM((A, nb_t, rank, cols), bf),
            pltpu.VMEM((nb_a, rank, BLOCK), bf),
            pltpu.VMEM((T, nb_t, rank, BLOCK), bf),
            dma((3,)), dma((np_,)),
            dma((2 * chips,)), dma((A,)),
            dma((A,)), dma((A,)), dma((A,)), dma((A,)),
            dma((A, nb_a)), dma((T, nb_t)),
            dma((T - 1, np_)), dma((T - 1, np_)), dma((T - 1, np_)), dma((T - 1, np_)),
        ],
        compiler_params=pltpu.CompilerParams(
            collective_id=0, has_side_effects=True, vmem_limit_bytes=60 * 1024 * 1024
        ),
    )(ids, live, slots, tokens, query_weight, down, up)


def solution(mesh):
    placed = (
        P(("groups", "adapter"), "tensor"),
        P("tensor", "adapter"),
        P("adapter", None, "tensor"),
        P("adapter", None, None),
        P("groups"),
        P("groups"),
        P("groups"),
    )
    return jax.shard_map(
        on_device,
        mesh=mesh,
        in_specs=placed,
        out_specs=P(("groups", "tensor"), "adapter"),
        check_vma=False,
    )
```
